32 devices in a mesh: freq: 4 (over y, x), space: 8 (over z, core).
Axes of the slice: x: 2, y: 2, z: 4, core: 2. Of those that a mesh axis runs over, the one named last changes fastest.
Arguments:
- snapshots: float32 [2, 256, 3, 4096], P(None, 'freq', None, 'space'), may hold values from -6 to 6
- mean_field: float32 [3, 4096], P(None, 'space'), may hold values from -3 to 3
- weights: float32 [3, 4096], P(None, 'space'), may hold values from 0.25 to 4
- rates: float32 [128], P('freq'), may hold values from 0.2 to 0.8
- modes: float32 [128, 2, 16, 3, 4096], P('freq', None, None, None, 'space'), may hold values from -6 to 6
Outputs:
- modes_out: float32 [128, 2, 16, 3, 4096], P('freq', None, None, None, 'space')
- coefficients: float32 [2, 128, 2, 16], P(None, 'freq')
The draws below stay inside these ranges and needn't reach their ends.
All inputs are finite; a program needn't handle non-finite values.
Results may differ from the reference program's by a relative error of at most 0.00024.
Values sent between devices are 32-bit elements; how exact they have to be, the bound alone decides.
No kernel may reach another device: no remote copies, remote signals or barrier semaphores. Data moves between devices by JAX's collectives and lax.ppermute only.
A program may use at most 64 MiB of HBM per device.

```python
import math
import jax
import jax.numpy as jnp
from jax import lax

NT = 256
NF = 128
K = 16
FIELDS = 3
BLOCKS = 2
POINTS = 4096


def steps_of(rng, shape, cuts, least, largest):
    level = 1.0
    for dim, blocks in cuts:
        heights = jax.random.uniform(jax.random.fold_in(jax.random.fold_in(rng, 6), dim), (blocks,), jnp.float32, least / len(cuts), largest / len(cuts))
        level = level * jnp.repeat(jnp.exp(heights), shape[dim] // blocks).reshape((-1,) + (1,) * (len(shape) - 1 - dim))
    return level


def scatter_about(key, dims, width, reach, split=(), held_as=jnp.bfloat16):
    values = width * jax.random.normal(key, dims, jnp.float32)
    if split:
        values = values * steps_of(key, dims, split, -0.22, 0.18)
    return jnp.clip(values, -reach, reach).astype(held_as)


def setup_inputs(seed: int = 0) -> dict:
    splits = jax.random.split(jax.random.key(seed), 6)
    snapshots = scatter_about(splits[0], (BLOCKS, NT, FIELDS, POINTS), 1.0, 6.0, ((1, 4), (3, 8)), jnp.float32)
    mean_field = scatter_about(splits[1], (FIELDS, POINTS), 0.5, 3.0, ((1, 8),), jnp.float32)
    weights = jnp.clip(jnp.exp(math.log(4.0) - 2.7725887 * jax.random.uniform(splits[2], (FIELDS, POINTS), jnp.float32) ** steps_of(splits[2], (FIELDS, POINTS), ((1, 8),), -0.2, 0.2)), 0.25, 4.0)
    rates = jnp.clip(jnp.exp(math.log(0.8) - 1.3862944 * jax.random.uniform(splits[3], (NF,), jnp.float32) ** steps_of(splits[3], (NF,), ((0, 4),), -0.2, 0.2)), 0.2, 0.8)
    modes = scatter_about(splits[4], (NF, 2, K, FIELDS, POINTS), 1.0, 6.0, ((0, 4), (4, 8)), jnp.float32)
    return dict(snapshots=snapshots, mean_field=mean_field, weights=weights, rates=rates, modes=modes)


def project(matrix, vector):
    return jnp.einsum('fkcp,fcp->fk', matrix, vector, precision=lax.Precision.HIGHEST)

def combine(coefs, matrix):
    return jnp.einsum('fk,fkcp->fcp', coefs, matrix, precision=lax.Precision.HIGHEST)

def reference(snapshots, mean_field, weights, rates, modes):
    times = jnp.arange(NT, dtype=jnp.float32)
    window = 0.5 - 0.5 * jnp.cos(2.0 * math.pi / NT * times)
    scale_factor = 1.0 / math.sqrt(3.0 * NT / 8.0)
    point_count = FIELDS * POINTS
    root_count = math.sqrt(point_count)
    modes_real = modes[:, 0]
    modes_imag = modes[:, 1]
    coef_list = []
    for block in range(BLOCKS):
        centered = (snapshots[block] - mean_field[None]) * window[:, None, None]
        spectra = jnp.fft.rfft(centered, axis=0)[:NF] * scale_factor
        spec_real = jnp.real(spectra).astype(jnp.float32)
        spec_imag = jnp.imag(spectra).astype(jnp.float32)
        weighted_real = weights[None] * spec_real
        weighted_imag = weights[None] * spec_imag
        coefs_real = (project(modes_real, weighted_real) + project(modes_imag, weighted_imag)) / root_count
        coefs_imag = (project(modes_real, weighted_imag) - project(modes_imag, weighted_real)) / root_count
        energy = lax.optimization_barrier(jnp.sum(weighted_real * spec_real + weighted_imag * spec_imag, axis=(1, 2))) / point_count
        coef_list.append(jnp.stack((coefs_real, coefs_imag), axis=1))
        resid_real = spec_real - (combine(coefs_real, modes_real) - combine(coefs_imag, modes_imag)) / root_count
        resid_imag = spec_imag - (combine(coefs_real, modes_imag) + combine(coefs_imag, modes_real)) / root_count
        gain = rates / jnp.sqrt(energy + 1e-06)
        steps_real = (gain[:, None] * coefs_real)[:, :, None, None]
        steps_imag = (-gain[:, None] * coefs_imag)[:, :, None, None]
        fresh_real = modes_real + steps_real * resid_real[:, None] - steps_imag * resid_imag[:, None]
        fresh_imag = modes_imag + steps_real * resid_imag[:, None] + steps_imag * resid_real[:, None]
        norms = lax.optimization_barrier(jnp.sum(weights[None, None] * (fresh_real * fresh_real + fresh_imag * fresh_imag), axis=(2, 3))) / point_count
        divisor = jnp.sqrt(norms + 1e-06)[:, :, None, None]
        modes_real = fresh_real / divisor
        modes_imag = fresh_imag / divisor
    return (jnp.stack((modes_real, modes_imag), axis=1), jnp.stack(coef_list, axis=0))
```

```python
import math

import jax
import jax.numpy as jnp
from jax import lax
from jax.experimental import pallas as pl
from jax.experimental.pallas import tpu as pltpu
from jax.sharding import PartitionSpec as P

EPS = 1e-06


def spectral_table(freq_ids, time_ids, length):
    phase = freq_ids[:, None] * time_ids[None, :] % length
    angle = 2.0 * math.pi / length * phase.astype(jnp.float32)
    window = 0.5 - 0.5 * jnp.cos(2.0 * math.pi / length * time_ids.astype(jnp.float32))
    weight_row = window / math.sqrt(3.0 * length / 8.0)
    return jnp.concatenate(
        (jnp.cos(angle) * weight_row[None], -jnp.sin(angle) * weight_row[None]), axis=0
    )


def split(value):
    high = value.astype(jnp.bfloat16)
    low = (value - high.astype(jnp.float32)).astype(jnp.bfloat16)
    return high, low


def nt_dot(left, right):
    return lax.dot_general(
        left, right, (((1,), (1,)), ((), ())), preferred_element_type=jnp.float32
    )


def gram_kernel(w_ref, m_ref, g_ref):
    fields = m_ref.shape[2]
    kk = m_ref.shape[3]

    def one(i, carry):
        total = jnp.zeros((2 * kk, 2 * kk), jnp.float32)
        for c in range(fields):
            root = jnp.sqrt(w_ref[c])
            both = jnp.concatenate((m_ref[i, 0, c] * root, m_ref[i, 1, c] * root), axis=0)
            high, low = split(both)
            total += nt_dot(high, high) + nt_dot(low, high) + nt_dot(high, low)
        g_ref[i, :, :kk] = total[:kk, :kk] + total[kk:, kk:]
        g_ref[i, :, kk:] = total[:kk, kk:] - total[kk:, :kk]
        return carry

    lax.fori_loop(0, m_ref.shape[0], one, 0)


def lane_sum(value):
    return jnp.sum(value, axis=1, keepdims=True)


def project_kernel(w_ref, q_ref, m_ref, p_ref):
    step = pl.program_id(0)
    per_step = m_ref.shape[0]
    fields = m_ref.shape[2]
    kk = m_ref.shape[3]
    count = q_ref.shape[3]
    lanes = p_ref.shape[1]

    @pl.when(step == 0)
    def _():
        p_ref[...] = jnp.zeros_like(p_ref)

    lane = lax.broadcasted_iota(jnp.int32, (kk, lanes), 1)
    lane_row = lax.broadcasted_iota(jnp.int32, (1, lanes), 1)

    def one(i, carry):
        f = step * per_step + i
        accs = [0.0] * 4
        rows = [0.0] * 4
        for c in range(fields):
            mr = m_ref[i, 0, c]
            mi = m_ref[i, 1, c]
            w = w_ref[c]
            qs = [q_ref[b, c, s, pl.ds(f, 1), :] for b in range(2) for s in range(2)]
            wq = [w * q for q in qs]
            for b in range(2):
                accs[2 * b] += mr * wq[2 * b] + mi * wq[2 * b + 1]
                accs[2 * b + 1] += mr * wq[2 * b + 1] - mi * wq[2 * b]
            rows[0] += wq[0] * qs[0] + wq[1] * qs[1]
            rows[1] += wq[2] * qs[2] + wq[3] * qs[3]
            rows[2] += wq[0] * qs[2] + wq[1] * qs[3]
            rows[3] += wq[0] * qs[3] - wq[1] * qs[2]
        tile = p_ref[:kk]
        row = p_ref[kk : kk + 1]
        for j in range(4):
            spot = j * count + f
            tile = jnp.where(lane == spot, lane_sum(accs[j]), tile)
            row = jnp.where(lane_row == spot, lane_sum(rows[j]), row)
        p_ref[:kk] = tile
        p_ref[kk : kk + 1] = row
        return carry

    lax.fori_loop(0, per_step, one, 0)


def small_math(g_ref, p_ref, rate_ref, coef_ref, tab_ref, point_count):
    kk = g_ref.shape[1]
    count = g_ref.shape[3]
    root = math.sqrt(point_count)
    total = p_ref[0]
    for s in range(1, p_ref.shape[0]):
        total = total + p_ref[s]
    part = [total[:kk, j * count : (j + 1) * count] for j in range(4)]
    row = [total[kk : kk + 1, j * count : (j + 1) * count] for j in range(4)]
    p0r, p0i, p1r, p1i = part
    e00, e11, xr, xi = row
    rate = rate_ref[...]

    def sum_k(value):
        return jnp.sum(value, axis=0, keepdims=True)

    def times_gram(hr, hi):
        vr = jnp.zeros((kk, count), jnp.float32)
        vi = jnp.zeros((kk, count), jnp.float32)
        for l in range(kk):
            gr = g_ref[0, l]
            gi = g_ref[1, l]
            ar = hr[l : l + 1]
            ai = hi[l : l + 1]
            vr += gr * ar - gi * ai
            vi += gr * ai + gi * ar
        return vr, vi

    sub = lax.broadcasted_iota(jnp.int32, (kk, count), 0)
    diag = jnp.zeros((kk, count), jnp.float32)
    for l in range(kk):
        diag = jnp.where(sub == l, g_ref[0, l], diag)

    a0r = p0r / root
    a0i = p0i / root
    gain0 = rate / jnp.sqrt(e00 / point_count + EPS)
    cr = gain0 * a0r
    ci = -gain0 * a0i
    br = a0r / root
    bi = a0i / root
    vr, vi = times_gram(br, bi)
    sr = p0r - vr
    si = p0i - vi
    t0 = e00 - sum_k(br * p0r + bi * p0i) - sum_k(sr * br + si * bi)
    t0 = jnp.maximum(t0, 0.0)
    n0 = diag + 2.0 * (cr * sr - ci * si) + (cr * cr + ci * ci) * t0
    n0 = jnp.maximum(n0, 0.0) / point_count
    d0 = 1.0 / jnp.sqrt(n0 + EPS)
    yr = xr - sum_k(br * p1r + bi * p1i)
    yi = xi - sum_k(br * p1i - bi * p1r)
    u1r = d0 * (p1r + cr * yr + ci * yi)
    u1i = d0 * (p1i + cr * yi - ci * yr)
    a1r = u1r / root
    a1i = u1i / root
    gain1 = rate / jnp.sqrt(e11 / point_count + EPS)
    er = gain1 * a1r
    ei = -gain1 * a1i
    b1r = a1r / root
    b1i = a1i / root
    hr = d0 * b1r
    hi = d0 * b1i
    bigr = sum_k(cr * hr - ci * hi)
    bigi = sum_k(cr * hi + ci * hr)
    zr = sum_k(sr * hr + si * hi)
    zi = sum_k(sr * hi - si * hr)
    vr, vi = times_gram(hr, hi)
    kr = zr + t0 * bigr
    ki = zi + t0 * bigi
    s1r = u1r - d0 * (vr + sr * bigr - si * bigi + cr * kr + ci * ki)
    s1i = u1i - d0 * (vi + sr * bigi + si * bigr + cr * ki - ci * kr)
    t1 = e11 - sum_k(b1r * u1r + b1i * u1i) - sum_k(s1r * b1r + s1i * b1i)
    t1 = jnp.maximum(t1, 0.0)
    n1 = d0 * d0 * n0 * point_count + 2.0 * (er * s1r - ei * s1i) + (er * er + ei * ei) * t1
    n1 = jnp.maximum(n1, 0.0) / point_count
    d1 = 1.0 / jnp.sqrt(n1 + EPS)
    both = d0 * d1
    coef_ref[0, 0] = a0r
    coef_ref[0, 1] = a0i
    coef_ref[1, 0] = a1r
    coef_ref[1, 1] = a1i
    wide = jnp.zeros((kk, count), jnp.float32)
    for n, value in enumerate(
        (br, bi, hr, hi, both, both * cr, both * ci, d1 * er, d1 * ei, wide + bigr, wide + bigi)
    ):
        tab_ref[n] = value


def update_kernel(g_ref, p_ref, rate_ref, q_ref, m_ref, out_ref, coef_ref, tab_ref, *, point_count):
    step = pl.program_id(0)
    per_step = m_ref.shape[0]
    fields = m_ref.shape[2]
    kk = m_ref.shape[3]
    count = q_ref.shape[3]

    @pl.when(step == 0)
    def _():
        small_math(g_ref, p_ref, rate_ref, coef_ref, tab_ref, point_count)

    lane = lax.broadcasted_iota(jnp.int32, (kk, count), 1)

    def one(i, carry):
        f = step * per_step + i
        here = lane == f
        cols = [lane_sum(jnp.where(here, tab_ref[n], 0.0)) for n in range(tab_ref.shape[0])]
        br, bi, hr, hi, ad, cr, ci, er, ei = cols[:9]
        bigr = cols[9][:1]
        bigi = cols[10][:1]
        for c in range(fields):
            mr = m_ref[i, 0, c]
            mi = m_ref[i, 1, c]
            q0r, q0i, q1r, q1i = [
                q_ref[b, c, s, pl.ds(f, 1), :] for b in range(2) for s in range(2)
            ]
            r0r = q0r - jnp.sum(br * mr - bi * mi, axis=0, keepdims=True)
            r0i = q0i - jnp.sum(br * mi + bi * mr, axis=0, keepdims=True)
            r1r = q1r - jnp.sum(hr * mr - hi * mi, axis=0, keepdims=True)
            r1i = q1i - jnp.sum(hr * mi + hi * mr, axis=0, keepdims=True)
            r1r = r1r - (bigr * r0r - bigi * r0i)
            r1i = r1i - (bigr * r0i + bigi * r0r)
            out_ref[i, 0, c] = ad * mr + (cr * r0r - ci * r0i) + (er * r1r - ei * r1i)
            out_ref[i, 1, c] = ad * mi + (cr * r0i + ci * r0r) + (er * r1i + ei * r1r)
        return carry

    lax.fori_loop(0, per_step, one, 0)


def share(value, axis):
    size = lax.axis_size(axis)
    return lax.all_to_all(
        jnp.broadcast_to(value[None], (size,) + value.shape), axis, 0, 0, tiled=True
    )


def per_device(snapshots, mean_field, weights, rates, modes):
    freq_count = lax.axis_size("freq")
    blocks, quarter, fields, points = snapshots.shape
    assert blocks == 2
    length = quarter * freq_count
    point_count = fields * points * lax.axis_size("space")
    count, _, kk = modes.shape[:3]
    per_step = math.gcd(count, 4)
    steps = count // per_step
    me = lax.axis_index("freq")
    snaps = snapshots.transpose(0, 2, 1, 3)
    ms = modes.transpose(0, 1, 3, 2, 4)
    w3 = weights[:, None, :]

    moved = [snaps]
    for m in range(1, freq_count):
        if freq_count & (freq_count - 1) == 0:
            pairs = [(i, i ^ m) for i in range(freq_count)]
        else:
            pairs = [(i, (i + m) % freq_count) for i in range(freq_count)]
        moved.append(lax.ppermute(snaps, "freq", pairs))

    m_spec = pl.BlockSpec((per_step, 2, fields, kk, points), lambda s: (s, 0, 0, 0, 0))
    w_spec = pl.BlockSpec((fields, 1, points), lambda s: (0, 0, 0))
    q_spec = pl.BlockSpec((blocks, fields, 2, count, points), lambda s: (0, 0, 0, 0, 0))

    gram = pl.pallas_call(
        gram_kernel,
        grid=(steps,),
        in_specs=[w_spec, m_spec],
        out_specs=pl.BlockSpec((per_step, kk, 2 * kk), lambda s: (s, 0, 0)),
        out_shape=jax.ShapeDtypeStruct((count, kk, 2 * kk), jnp.float32),
        name="gram",
    )(w3, ms)
    gram = jnp.sum(share(gram.reshape(count * kk * 2 * kk // 128, 128), "space"), axis=0)
    gram = gram.reshape(count, kk, 2, kk).transpose(2, 3, 1, 0)

    freq_ids = me * count + jnp.arange(count, dtype=jnp.int32)
    spectra = 0.0
    for m in range(freq_count):
        if freq_count & (freq_count - 1) == 0:
            source = me ^ m
        else:
            source = (me - m) % freq_count
        times = source * quarter + jnp.arange(quarter, dtype=jnp.int32)
        table = spectral_table(freq_ids, times, length)
        spectra = spectra + jnp.einsum(
            "rt,bctp->bcrp",
            table,
            moved[m] - mean_field[None, :, None, :],
            precision=lax.Precision.HIGHEST,
        )
    spectra = spectra.reshape(blocks, fields, 2, count, points)

    rows = -(-(kk + 1) // 8) * 8
    lanes = 4 * count
    prods = pl.pallas_call(
        project_kernel,
        grid=(steps,),
        in_specs=[w_spec, q_spec, m_spec],
        out_specs=pl.BlockSpec((rows, lanes), lambda s: (0, 0)),
        out_shape=jax.ShapeDtypeStruct((rows, lanes), jnp.float32),
        name="project",
    )(w3, spectra, ms)
    prods = share(prods, "space")

    def full(shape):
        return pl.BlockSpec(shape, lambda s: (0,) * len(shape))

    out, coefs = pl.pallas_call(
        lambda *refs: update_kernel(*refs, point_count=point_count),
        grid=(steps,),
        in_specs=[full(gram.shape), full(prods.shape), full((1, count)), q_spec, m_spec],
        out_specs=[m_spec, full((blocks, 2, kk, count))],
        out_shape=[
            jax.ShapeDtypeStruct(ms.shape, jnp.float32),
            jax.ShapeDtypeStruct((blocks, 2, kk, count), jnp.float32),
        ],
        scratch_shapes=[pltpu.VMEM((11, kk, count), jnp.float32)],
        name="update",
    )(gram, prods, rates[None], spectra, ms)
    return out.transpose(0, 1, 3, 2, 4), coefs.transpose(0, 3, 1, 2)


def solution(mesh):
    return jax.shard_map(
        per_device,
        mesh=mesh,
        in_specs=(
            P(None, "freq", None, "space"),
            P(None, "space"),
            P(None, "space"),
            P("freq"),
            P("freq", None, None, None, "space"),
        ),
        out_specs=(P("freq", None, None, None, "space"), P(None, "freq", None, None)),
        check_vma=False,
    )
```

```python
import math

import jax
import jax.numpy as jnp
from jax import lax
from jax.experimental import pallas as pl
from jax.experimental.pallas import tpu as pltpu
from jax.sharding import PartitionSpec as P

EPS = 1e-06


def spectral_table(freq_ids, time_ids, length):
    phase = freq_ids[:, None] * time_ids[None, :] % length
    angle = 2.0 * math.pi / length * phase.astype(jnp.float32)
    window = 0.5 - 0.5 * jnp.cos(2.0 * math.pi / length * time_ids.astype(jnp.float32))
    weight_row = window / math.sqrt(3.0 * length / 8.0)
    return jnp.concatenate(
        (jnp.cos(angle) * weight_row[None], -jnp.sin(angle) * weight_row[None]), axis=0
    )


def split(value):
    high = value.astype(jnp.bfloat16)
    low = (value - high.astype(jnp.float32)).astype(jnp.bfloat16)
    return high, low


def nt_dot(left, right):
    return lax.dot_general(
        left, right, (((1,), (1,)), ((), ())), preferred_element_type=jnp.float32
    )


def rolled(number, one, carry):
    some = math.gcd(number, 4)

    def several(j, carry):
        for i in range(some):
            carry = one(j * some + i, carry)
        return carry

    return lax.fori_loop(0, number // some, several, carry)


def gram_kernel(w_ref, m_ref, g_ref):
    fields = m_ref.shape[2]
    kk = m_ref.shape[3]
    roots = [jnp.sqrt(w_ref[c : c + 1]) for c in range(fields)]

    def one(i, carry):
        total = jnp.zeros((2 * kk, 2 * kk), jnp.float32)
        for c in range(fields):
            both = jnp.concatenate((m_ref[i, 0, c] * roots[c], m_ref[i, 1, c] * roots[c]), axis=0)
            high, low = split(both)
            total += nt_dot(high, high) + nt_dot(low, high) + nt_dot(high, low)
        g_ref[i, :, :kk] = total[:kk, :kk] + total[kk:, kk:]
        g_ref[i, :, kk:] = total[:kk, kk:] - total[kk:, :kk]
        return carry

    rolled(m_ref.shape[0], one, 0)


def lane_sum(value):
    return jnp.sum(value, axis=1, keepdims=True)


def places(number, width):
    me = lax.axis_index("freq")
    return [
        pl.ds(pl.multiple_of(partner_of(me, m, number) * width, width), width)
        for m in range(number)
    ]


def pack_kernel(mean_ref, x_ref, *out_refs):
    width = out_refs[0].shape[3]
    for here, out_ref in zip(places(len(out_refs), width), out_refs):
        for c in range(x_ref.shape[1]):
            out_ref[0, c] = x_ref[0, c, :, here] - mean_ref[c : c + 1, here]


def spectra_kernel(table_ref, *refs):
    number = len(refs) // 2
    in_refs, out_refs = refs[:number], refs[number:]
    th, tl = split(table_ref[...])
    fields = in_refs[0].shape[1]
    _, _, _, count, width = out_refs[0].shape
    for c in range(fields):
        xh, xl = split(jnp.concatenate([ref[0, c] for ref in in_refs], axis=0))
        out = nn_dot(th, xh) + nn_dot(tl, xh) + nn_dot(th, xl)
        out = out.reshape(number, 2, count, width)
        for m in range(number):
            out_refs[m][0, c] = out[m]


def nn_dot(left, right):
    return jnp.dot(left, right, preferred_element_type=jnp.float32)


def project_kernel(w_ref, *refs):
    *q_refs, m_ref, p_ref = refs
    step = pl.program_id(0)
    per_step = m_ref.shape[0]
    fields = m_ref.shape[2]
    kk = m_ref.shape[3]
    count, width = q_refs[0].shape[3:]
    lanes = p_ref.shape[1]

    @pl.when(step == 0)
    def _():
        p_ref[...] = jnp.zeros_like(p_ref)

    lane = lax.broadcasted_iota(jnp.int32, (kk, lanes), 1)
    lane_row = lax.broadcasted_iota(jnp.int32, (1, lanes), 1)
    spots = places(len(q_refs), width)

    def one(i, carry):
        tile, row = carry
        f = step * per_step + i
        accs = [0.0] * 4
        rows = [0.0] * 4
        for here, q_ref in zip(spots, q_refs):
            for c in range(fields):
                mr = m_ref[i, 0, c, :, here]
                mi = m_ref[i, 1, c, :, here]
                w = w_ref[c : c + 1, here]
                qs = [q_ref[b, c, s, pl.ds(f, 1), :] for b in range(2) for s in range(2)]
                wq = [w * q for q in qs]
                for b in range(2):
                    accs[2 * b] += mr * wq[2 * b] + mi * wq[2 * b + 1]
                    accs[2 * b + 1] += mr * wq[2 * b + 1] - mi * wq[2 * b]
                rows[0] += wq[0] * qs[0] + wq[1] * qs[1]
                rows[1] += wq[2] * qs[2] + wq[3] * qs[3]
                rows[2] += wq[0] * qs[2] + wq[1] * qs[3]
                rows[3] += wq[0] * qs[3] - wq[1] * qs[2]
        for j in range(4):
            spot = j * count + f
            tile = jnp.where(lane == spot, lane_sum(accs[j]), tile)
            row = jnp.where(lane_row == spot, lane_sum(rows[j]), row)
        return tile, row

    tile, row = rolled(per_step, one, (p_ref[:kk], p_ref[kk : kk + 1]))
    p_ref[:kk] = tile
    p_ref[kk : kk + 1] = row


def small_math(g_ref, p_ref, rate_ref, coef_ref, tab_ref, point_count):
    kk = g_ref.shape[1]
    count = g_ref.shape[3]
    root = math.sqrt(point_count)
    total = p_ref[...]
    part = [total[:kk, j * count : (j + 1) * count] for j in range(4)]
    row = [total[kk : kk + 1, j * count : (j + 1) * count] for j in range(4)]
    p0r, p0i, p1r, p1i = part
    e00, e11, xr, xi = row
    rate = rate_ref[...]

    def sum_k(value):
        return jnp.sum(value, axis=0, keepdims=True)

    def times_gram(hr, hi):
        vr = jnp.zeros((kk, count), jnp.float32)
        vi = jnp.zeros((kk, count), jnp.float32)
        for l in range(kk):
            gr = g_ref[0, l]
            gi = g_ref[1, l]
            ar = hr[l : l + 1]
            ai = hi[l : l + 1]
            vr += gr * ar - gi * ai
            vi += gr * ai + gi * ar
        return vr, vi

    sub = lax.broadcasted_iota(jnp.int32, (kk, count), 0)
    diag = jnp.zeros((kk, count), jnp.float32)
    for l in range(kk):
        diag = jnp.where(sub == l, g_ref[0, l], diag)

    a0r = p0r / root
    a0i = p0i / root
    gain0 = rate / jnp.sqrt(e00 / point_count + EPS)
    cr = gain0 * a0r
    ci = -gain0 * a0i
    br = a0r / root
    bi = a0i / root
    vr, vi = times_gram(br, bi)
    sr = p0r - vr
    si = p0i - vi
    t0 = e00 - sum_k(br * p0r + bi * p0i) - sum_k(sr * br + si * bi)
    t0 = jnp.maximum(t0, 0.0)
    n0 = diag + 2.0 * (cr * sr - ci * si) + (cr * cr + ci * ci) * t0
    n0 = jnp.maximum(n0, 0.0) / point_count
    d0 = 1.0 / jnp.sqrt(n0 + EPS)
    yr = xr - sum_k(br * p1r + bi * p1i)
    yi = xi - sum_k(br * p1i - bi * p1r)
    u1r = d0 * (p1r + cr * yr + ci * yi)
    u1i = d0 * (p1i + cr * yi - ci * yr)
    a1r = u1r / root
    a1i = u1i / root
    gain1 = rate / jnp.sqrt(e11 / point_count + EPS)
    er = gain1 * a1r
    ei = -gain1 * a1i
    b1r = a1r / root
    b1i = a1i / root
    hr = d0 * b1r
    hi = d0 * b1i
    bigr = sum_k(cr * hr - ci * hi)
    bigi = sum_k(cr * hi + ci * hr)
    zr = sum_k(sr * hr + si * hi)
    zi = sum_k(sr * hi - si * hr)
    vr, vi = times_gram(hr, hi)
    kr = zr + t0 * bigr
    ki = zi + t0 * bigi
    s1r = u1r - d0 * (vr + sr * bigr - si * bigi + cr * kr + ci * ki)
    s1i = u1i - d0 * (vi + sr * bigi + si * bigr + cr * ki - ci * kr)
    t1 = e11 - sum_k(b1r * u1r + b1i * u1i) - sum_k(s1r * b1r + s1i * b1i)
    t1 = jnp.maximum(t1, 0.0)
    n1 = d0 * d0 * n0 * point_count + 2.0 * (er * s1r - ei * s1i) + (er * er + ei * ei) * t1
    n1 = jnp.maximum(n1, 0.0) / point_count
    d1 = 1.0 / jnp.sqrt(n1 + EPS)
    both = d0 * d1
    coef_ref[0, 0] = a0r
    coef_ref[0, 1] = a0i
    coef_ref[1, 0] = a1r
    coef_ref[1, 1] = a1i
    wide = jnp.zeros((kk, count), jnp.float32)
    for n, value in enumerate(
        (br, bi, hr, hi, both, both * cr, both * ci, d1 * er, d1 * ei, wide + bigr, wide + bigi)
    ):
        tab_ref[n] = value


def update_kernel(g_ref, p_ref, rate_ref, *refs, point_count):
    *q_refs, m_ref, out_ref, coef_ref, tab_ref = refs
    step = pl.program_id(0)
    per_step = m_ref.shape[0]
    fields = m_ref.shape[2]
    kk = m_ref.shape[3]
    count, width = q_refs[0].shape[3:]

    @pl.when(step == 0)
    def _():
        small_math(g_ref, p_ref, rate_ref, coef_ref, tab_ref, point_count)

    lane = lax.broadcasted_iota(jnp.int32, (kk, count), 1)

    spots = places(len(q_refs), width)

    def one(i, carry):
        f = step * per_step + i
        here = lane == f
        cols = [lane_sum(jnp.where(here, tab_ref[n], 0.0)) for n in range(tab_ref.shape[0])]
        br, bi, hr, hi, ad, cr, ci, er, ei = [
            jnp.broadcast_to(col, (kk, width)) for col in cols[:9]
        ]
        bigr = cols[9][:1]
        bigi = cols[10][:1]
        for spot, q_ref in zip(spots, q_refs):
            for c in range(fields):
                mr = m_ref[i, 0, c, :, spot]
                mi = m_ref[i, 1, c, :, spot]
                q0r, q0i, q1r, q1i = [
                    q_ref[b, c, s, pl.ds(f, 1), :] for b in range(2) for s in range(2)
                ]
                r0r = q0r - jnp.sum(br * mr - bi * mi, axis=0, keepdims=True)
                r0i = q0i - jnp.sum(br * mi + bi * mr, axis=0, keepdims=True)
                r1r = q1r - jnp.sum(hr * mr - hi * mi, axis=0, keepdims=True)
                r1i = q1i - jnp.sum(hr * mi + hi * mr, axis=0, keepdims=True)
                r1r = r1r - (bigr * r0r - bigi * r0i)
                r1i = r1i - (bigr * r0i + bigi * r0r)
                out_ref[i, 0, c, :, spot] = ad * mr + (cr * r0r - ci * r0i) + (er * r1r - ei * r1i)
                out_ref[i, 1, c, :, spot] = ad * mi + (cr * r0i + ci * r0r) + (er * r1i + ei * r1r)
        return carry

    rolled(per_step, one, 0)


def total_of(value, axis):
    size = lax.axis_size(axis)
    if size & (size - 1):
        wide = jnp.broadcast_to(value[None], (size,) + value.shape)
        return jnp.sum(lax.all_to_all(wide, axis, 0, 0, tiled=True), axis=0)
    hop = 1
    while hop < size:
        value = value + lax.ppermute(value, axis, [(i, i ^ hop) for i in range(size)])
        hop *= 2
    return value


def partner_of(me, m, size):
    return me ^ m if size & (size - 1) == 0 else (m - me) % size


def exchange(parts, axis):
    size = lax.axis_size(axis)
    out = []
    for m, part in enumerate(parts):
        pairs = [(i, partner_of(i, m, size)) for i in range(size)]
        same = all(i == j for i, j in pairs)
        out.append(part if same else lax.ppermute(part, axis, pairs))
    return out


def full(shape):
    return pl.BlockSpec(shape, lambda s: (0,) * len(shape))


def lead(shape):
    return pl.BlockSpec((1,) + shape[1:], lambda s: (s,) + (0,) * (len(shape) - 1))


def per_device(snapshots, mean_field, weights, rates, modes):
    ways = lax.axis_size("freq")
    blocks, quarter, fields, points = snapshots.shape
    assert blocks == 2
    length = quarter * ways
    point_count = fields * points * lax.axis_size("space")
    count, _, kk = modes.shape[:3]
    width = points // ways
    per_step = math.gcd(count, 8)
    steps = count // per_step
    me = lax.axis_index("freq").astype(jnp.int32)
    snaps = snapshots.transpose(0, 2, 1, 3)
    ms = modes.transpose(0, 1, 3, 2, 4)
    partners = jnp.stack([partner_of(me, m, ways) for m in range(ways)]).astype(jnp.int32)

    cut = (blocks, fields, quarter, width)
    parts = pl.pallas_call(
        pack_kernel,
        grid=(blocks,),
        in_specs=[full((fields, points)), lead(snaps.shape)],
        out_specs=[lead(cut)] * ways,
        out_shape=[jax.ShapeDtypeStruct(cut, jnp.float32)] * ways,
        name="pack",
    )(mean_field, snaps)
    parts = exchange(parts, "freq")

    m_spec = pl.BlockSpec((per_step, 2, fields, kk, points), lambda s: (s, 0, 0, 0, 0))
    w_spec = full((fields, points))
    gram = pl.pallas_call(
        gram_kernel,
        grid=(steps,),
        in_specs=[w_spec, m_spec],
        out_specs=pl.BlockSpec((per_step, kk, 2 * kk), lambda s: (s, 0, 0)),
        out_shape=jax.ShapeDtypeStruct((count, kk, 2 * kk), jnp.float32),
        name="gram",
    )(weights, ms)

    freq_ids = partners[:, None] * count + jnp.arange(count, dtype=jnp.int32)[None]
    time_ids = partners[:, None] * quarter + jnp.arange(quarter, dtype=jnp.int32)[None]
    table = spectral_table(freq_ids.reshape(-1), time_ids.reshape(-1), length)
    table = table.reshape(2, ways, count, length).transpose(1, 0, 2, 3)
    table = table.reshape(2 * ways * count, length)
    cut = (blocks, fields, 2, count, width)
    gram, table, *parts = lax.optimization_barrier((gram, table, *parts))
    spectra = pl.pallas_call(
        spectra_kernel,
        grid=(blocks,),
        in_specs=[full(table.shape)] + [lead(parts[0].shape)] * ways,
        out_specs=[lead(cut)] * ways,
        out_shape=[jax.ShapeDtypeStruct(cut, jnp.float32)] * ways,
        name="spectra",
    )(table, *parts)
    spectra = exchange(spectra, "freq")

    gram = total_of(gram.reshape(count * kk * 2 * kk // 128, 128), "space")
    gram = gram.reshape(count, kk, 2, kk).transpose(2, 3, 1, 0)

    rows = -(-(kk + 1) // 8) * 8
    lanes = 4 * count
    q_specs = [full(cut)] * ways
    prods = pl.pallas_call(
        project_kernel,
        grid=(steps,),
        in_specs=[w_spec] + q_specs + [m_spec],
        out_specs=full((rows, lanes)),
        out_shape=jax.ShapeDtypeStruct((rows, lanes), jnp.float32),
        name="project",
    )(weights, *spectra, ms)
    prods = total_of(prods, "space")

    out, coefs = pl.pallas_call(
        lambda *refs: update_kernel(*refs, point_count=point_count),
        grid=(steps,),
        in_specs=[full(gram.shape), full(prods.shape), full((1, count))]
        + q_specs
        + [m_spec],
        out_specs=[m_spec, full((blocks, 2, kk, count))],
        out_shape=[
            jax.ShapeDtypeStruct(ms.shape, jnp.float32),
            jax.ShapeDtypeStruct((blocks, 2, kk, count), jnp.float32),
        ],
        scratch_shapes=[pltpu.VMEM((11, kk, count), jnp.float32)],
        name="update",
    )(gram, prods, rates[None], *spectra, ms)
    return out.transpose(0, 1, 3, 2, 4), coefs.transpose(0, 3, 1, 2)


def solution(mesh):
    return jax.shard_map(
        per_device,
        mesh=mesh,
        in_specs=(
            P(None, "freq", None, "space"),
            P(None, "space"),
            P(None, "space"),
            P("freq"),
            P("freq", None, None, None, "space"),
        ),
        out_specs=(P("freq", None, None, None, "space"), P(None, "freq", None, None)),
        check_vma=False,
    )
```
